32 devices in a mesh: pi: 4 (over y, x), pj: 8 (over z, core).
Axes of the slice: x: 2, y: 2, z: 4, core: 2. Of those that a mesh axis runs over, the one named last changes fastest.
Arguments:
- duo_embedding: bfloat16 [1024, 1024, 128], P('pi', 'pj'), may hold values from -12 to 12
- duo_attention_weights: float32 [128, 8], replicated, may hold values from -16 to 16
- aligned_embedding: bfloat16 [256, 64, 1024], P('pj', None, 'pi'), may hold values from -6 to 6
- aligned_scaling_weights: float32 [64], replicated, may hold values from 0.5 to 1.5
- aligned_shift_vector: float32 [64], replicated, may hold values from -3 to 3
- payload_weights: bfloat16 [64, 256], replicated, may hold values from -0.75 to 0.75
- switch_weights: bfloat16 [64, 256], replicated, may hold values from -0.75 to 0.75
- closing_weights: bfloat16 [256, 64], replicated, may hold values from -1.5 to 1.5
Outputs:
- update: bfloat16 [256, 64, 1024], P('pj', None, 'pi')
The draws below stay inside these ranges and needn't reach their ends.
All inputs are finite; a program needn't handle non-finite values.
Results may differ from the reference program's by a relative error of at most 0.009.
Values may be sent and summed in bfloat16 or wider, within the bound.
A program may use at most 192 MiB of HBM per device.

```python
import math
import jax
import jax.numpy as jnp
from jax import lax

ALIGNED_EMBED = 64
CZ = 128
ATTENDER_TALLY = 8
UNIT_SPAN = 32
POSITION_TALLY = 1024
ALIGNED_SEQS = 256
JOINT_SPAN = 256


def head_directions(key):
    random_dirs = jax.random.normal(jax.random.fold_in(key, 7001), (ATTENDER_TALLY, CZ), jnp.float32)
    random_dirs = random_dirs - jnp.mean(random_dirs, axis=1, keepdims=True)
    return random_dirs / jnp.sqrt(jnp.sum(random_dirs * random_dirs, axis=1, keepdims=True))


def score_weights(key):
    directions = head_directions(key)
    noise = jnp.clip(jax.random.normal(jax.random.fold_in(key, 7002), (CZ, ATTENDER_TALLY), jnp.float32), -6.0, 6.0)
    return 0.18 * noise + 0.35 * directions.T


def draw_duo_attention_weights(key, part):
    return score_weights(key)


def draw_duo_embedding(key, part):
    directions = head_directions(key)
    noise = jnp.clip(jax.random.normal(jax.random.fold_in(key, 7003), (POSITION_TALLY, POSITION_TALLY, CZ), jnp.float32), -6.0, 6.0)
    column_ramp = 2.0 * (2.0 * jnp.arange(POSITION_TALLY, dtype=jnp.float32) / (POSITION_TALLY - 1) - 1.0)
    pair_field = noise + column_ramp[None, :, None] * jnp.sum(directions, axis=0)[None, None, :]
    return pair_field.astype(jnp.bfloat16)


def level_of(key, extent, shards, least, high):
    loudness = 1.0
    for position, blocks in shards:
        heights = jax.random.uniform(jax.random.fold_in(jax.random.fold_in(key, 6), position), (blocks,), jnp.float32, least / len(shards), high / len(shards))
        loudness = loudness * jnp.repeat(jnp.exp(heights), extent[position] // blocks).reshape((-1,) + (1,) * (len(extent) - 1 - position))
    return loudness


def scatter_about(stream_key, extent, width, reach, cuts=(), kind=jnp.bfloat16):
    factor_of = level_of(stream_key, extent, cuts, -0.22, 0.18) if cuts else 1.0
    array = jax.random.normal(stream_key, extent, jnp.float32) * width * factor_of
    return jnp.minimum(jnp.maximum(array, -reach), reach).astype(kind)


def setup_inputs(seed: int = 0) -> dict:
    streams_of = jax.random.split(jax.random.key(seed), 9)
    return {
        "duo_embedding": draw_duo_embedding(jax.random.fold_in(streams_of[8], 71), 0),
        "duo_attention_weights": draw_duo_attention_weights(jax.random.fold_in(streams_of[8], 71), 0),
        "aligned_embedding": scatter_about(streams_of[2], (ALIGNED_SEQS, ALIGNED_EMBED, POSITION_TALLY), 1.0, 6.0, ((0, 8), (2, 4))),
        "aligned_scaling_weights": jnp.clip(1.0 + 0.1 * jax.random.normal(streams_of[3], (ALIGNED_EMBED,), jnp.float32), 0.5, 1.5),
        "aligned_shift_vector": scatter_about(streams_of[4], (ALIGNED_EMBED,), 0.5, 3.0, (), jnp.float32),
        "payload_weights": scatter_about(streams_of[5], (ALIGNED_EMBED, JOINT_SPAN), ALIGNED_EMBED ** -0.5, 0.75),
        "switch_weights": scatter_about(streams_of[6], (ALIGNED_EMBED, JOINT_SPAN), ALIGNED_EMBED ** -0.5, 0.75),
        "closing_weights": scatter_about(streams_of[7], (JOINT_SPAN, ALIGNED_EMBED), (JOINT_SPAN // 16) ** -0.5, 1.5),
    }


EPS = 1e-05

def rescale_embedding(inputs, axis):
    row_mean = lax.optimization_barrier(jnp.mean(inputs, axis=axis, keepdims=True))
    centred = inputs - row_mean
    variance = lax.optimization_barrier(jnp.mean(centred * centred, axis=axis, keepdims=True))
    return centred * lax.rsqrt(variance + EPS)

def reference(duo_embedding, duo_attention_weights, aligned_embedding, aligned_scaling_weights, aligned_shift_vector, payload_weights, switch_weights, closing_weights):
    aligned_fullbit_copy = aligned_embedding.astype(jnp.float32)
    rescaled_aligned = (rescale_embedding(aligned_fullbit_copy, 1) * aligned_scaling_weights[None, :, None] + aligned_shift_vector[None, :, None]).astype(jnp.bfloat16)
    normed_float = rescaled_aligned.astype(jnp.float32)
    payloads = jnp.einsum('scn,ce->sen', normed_float, payload_weights.astype(jnp.float32)).astype(jnp.bfloat16)
    switch_share = jax.nn.sigmoid(jnp.einsum('scn,ce->sen', normed_float, switch_weights.astype(jnp.float32)))
    payload_each_attender = payloads.astype(jnp.float32).reshape(ALIGNED_SEQS, ATTENDER_TALLY, UNIT_SPAN, POSITION_TALLY)
    tile_entries = math.gcd(POSITION_TALLY, 256)
    block_count = POSITION_TALLY // tile_entries

    def one_block(block_index):
        start_position = (block_index * tile_entries).astype(jnp.int32)
        pair_tile = lax.dynamic_slice_in_dim(duo_embedding, start_position, tile_entries, 0).astype(jnp.float32)
        pair_normed = rescale_embedding(pair_tile, 2)
        scores = jnp.einsum('ijc,ch->hij', pair_normed, duo_attention_weights, precision=lax.Precision.HIGHEST)
        row_peak = lax.optimization_barrier(jnp.max(scores, axis=2, keepdims=True))
        exp_scores = jnp.exp(scores - row_peak).astype(jnp.bfloat16)
        exp_float = exp_scores.astype(jnp.float32)
        row_total = lax.optimization_barrier(jnp.sum(exp_float, axis=2))
        numerator = jnp.einsum('hij,shcj->shci', exp_float, payload_each_attender)
        switch_tile = lax.dynamic_slice_in_dim(switch_share, start_position, tile_entries, 2).reshape(ALIGNED_SEQS, ATTENDER_TALLY, UNIT_SPAN, tile_entries)
        averaged_result = (switch_tile * (numerator / row_total[None, :, None, :])).astype(jnp.bfloat16)
        averaged_result = averaged_result.reshape(ALIGNED_SEQS, ATTENDER_TALLY * UNIT_SPAN, tile_entries).astype(jnp.float32)
        return jnp.einsum('ser,ec->scr', averaged_result, closing_weights.astype(jnp.float32)).astype(jnp.bfloat16)
    result_tiles = lax.map(one_block, jnp.arange(block_count, dtype=jnp.int32))
    return jnp.transpose(result_tiles, (1, 2, 0, 3)).reshape(ALIGNED_SEQS, ALIGNED_EMBED, POSITION_TALLY)
```

```python
import functools

import jax
import jax.numpy as jnp
from jax import lax
from jax.experimental import pallas as pl
from jax.experimental.pallas import tpu as pltpu
from jax.sharding import PartitionSpec as P

EPS = 1e-05
NT = (((1,), (1,)), ((), ()))


def dot(a, b, dims=(((1,), (0,)), ((), ()))):
    return lax.dot_general(a, b, dims, preferred_element_type=jnp.float32)


def rescale_embedding(inputs, axis):
    row_mean = jnp.mean(inputs, axis=axis, keepdims=True)
    centred = inputs - row_mean
    variance = jnp.mean(centred * centred, axis=axis, keepdims=True)
    return centred * lax.rsqrt(variance + EPS)


def pair_kernel(x_ref, w_ref, e_ref, m_ref, hold):
    rows, cols, chans = x_ref.shape
    heads = w_ref.shape[0]
    step = pl.program_id(0)
    w = w_ref[...]
    w = w - jnp.mean(w, axis=1, keepdims=True)
    hi = w.astype(jnp.bfloat16).astype(jnp.float32)
    mid = (w - hi).astype(jnp.bfloat16).astype(jnp.float32)
    w3 = jnp.concatenate([hi, mid, w - hi - mid, jnp.zeros_like(w)], axis=0)
    w3 = w3.astype(jnp.bfloat16)
    x = x_ref[...].reshape(rows * cols, chans)
    mean = dot(x, jnp.ones((chans, chans), jnp.bfloat16)) * (1.0 / chans)
    centred = x.astype(jnp.float32) - mean
    square = centred * centred
    top = square.astype(jnp.bfloat16)
    rest = (square - top.astype(jnp.float32)).astype(jnp.bfloat16)
    ones = jnp.ones((2 * heads, 2 * chans), jnp.bfloat16)
    variance = dot(ones, jnp.concatenate([top, rest], axis=1), NT)[:heads] * (1.0 / chans)
    parts = dot(w3, x, NT)
    scores = parts[:heads] + (parts[heads : 2 * heads] + parts[2 * heads : 3 * heads])
    scores = scores * lax.rsqrt(variance + EPS)
    lane = lax.broadcasted_iota(jnp.int32, m_ref.shape, 1)
    peaks = m_ref[...]
    for k in range(rows):
        one = scores[:, k * cols : (k + 1) * cols]
        peak = jnp.max(one, axis=1, keepdims=True)
        hold[:, k, :] = jnp.exp(one - peak)
        peaks = jnp.where(lane == step * rows + k, peak, peaks)
    m_ref[...] = peaks
    e_ref[...] = hold[...].astype(jnp.bfloat16)


def pair_call(duo, weights_t):
    rows, cols, chans = duo.shape
    heads = weights_t.shape[0]
    tile = 16
    return pl.pallas_call(
        pair_kernel,
        grid=(rows // tile,),
        in_specs=[
            pl.BlockSpec((tile, cols, chans), lambda i: (i, 0, 0)),
            pl.BlockSpec((heads, chans), lambda i: (0, 0)),
        ],
        out_specs=[
            pl.BlockSpec((heads, tile, cols), lambda i: (0, i, 0)),
            pl.BlockSpec((heads, rows), lambda i: (0, 0)),
        ],
        out_shape=[
            jax.ShapeDtypeStruct((heads, rows, cols), jnp.bfloat16),
            jax.ShapeDtypeStruct((heads, rows), jnp.float32),
        ],
        scratch_shapes=[pltpu.VMEM((heads, tile, cols), jnp.float32)],
        compiler_params=pltpu.CompilerParams(
            dimension_semantics=("arbitrary",), vmem_limit_bytes=40 << 20
        ),
        cost_estimate=pl.CostEstimate(
            flops=4 * 10**9, bytes_accessed=duo.size * 2, transcendentals=0
        ),
        name="pair",
    )(duo, weights_t)


def join_kernel(per_row, *refs):
    *blocks, scale_ref, w_ref, total_ref = refs
    cols = blocks[0].shape[2]
    me_i, me_j = lax.axis_index("pi"), lax.axis_index("pj")
    for r, block in enumerate(blocks):
        owner = me_j ^ r
        place = (lax.div(owner, per_row) ^ me_i) * per_row + lax.rem(owner, per_row)
        scaled = block[0].astype(jnp.float32) * scale_ref[0][:, r : r + 1]
        w_ref[0, :, pl.ds(pl.multiple_of(place * cols, cols), cols)] = scaled.astype(jnp.bfloat16)
    total_ref[0] = dot(jnp.ones((8, w_ref.shape[2]), jnp.bfloat16), w_ref[0], NT)


def join_call(blocks, scale, per_row):
    heads, rows, cols = blocks[0].shape
    count = len(blocks)
    return pl.pallas_call(
        functools.partial(join_kernel, per_row),
        grid=(heads,),
        in_specs=[pl.BlockSpec((1, rows, cols), lambda h: (h, 0, 0))] * count
        + [pl.BlockSpec((1, rows, count), lambda h: (h, 0, 0))],
        out_specs=[
            pl.BlockSpec((1, rows, count * cols), lambda h: (h, 0, 0)),
            pl.BlockSpec((1, 8, rows), lambda h: (h, 0, 0)),
        ],
        out_shape=[
            jax.ShapeDtypeStruct((heads, rows, count * cols), jnp.bfloat16),
            jax.ShapeDtypeStruct((heads, 8, rows), jnp.float32),
        ],
        compiler_params=pltpu.CompilerParams(
            dimension_semantics=("arbitrary",), vmem_limit_bytes=24 << 20
        ),
        name="join",
    )(*blocks, scale)


def body(
    pi_count,
    pj_count,
    duo_embedding,
    duo_attention_weights,
    aligned_embedding,
    aligned_scaling_weights,
    aligned_shift_vector,
    payload_weights,
    switch_weights,
    closing_weights,
):
    attender_tally = duo_attention_weights.shape[1]
    entry_tally = duo_embedding.shape[0]
    aligned_seq_tally = aligned_embedding.shape[0]
    inner_embed_size = payload_weights.shape[1]
    attender_span = inner_embed_size // attender_tally

    def swap(array, axis, count, bit):
        return lax.ppermute(array, axis, [(q, q ^ bit) for q in range(count)])

    rescaled_aligned = (
        rescale_embedding(aligned_embedding.astype(jnp.float32), 1)
        * aligned_scaling_weights[None, :, None]
        + aligned_shift_vector[None, :, None]
    ).astype(jnp.bfloat16)
    aligned_blocks = [rescaled_aligned] + [
        swap(rescaled_aligned, "pi", pi_count, r) for r in range(1, pi_count)
    ]

    exp_scores, peaks = pair_call(duo_embedding, duo_attention_weights.T)
    near = [exp_scores] + [swap(exp_scores, "pj", pj_count, r) for r in range(2, pj_count, 2)]
    near_peaks = [peaks] + [swap(peaks, "pj", pj_count, r) for r in range(2, pj_count, 2)]
    far = [swap(block, "pj", pj_count, 1) for block in near]
    near_peaks = jnp.stack(near_peaks)
    far_peaks = swap(near_peaks, "pj", pj_count, 1)
    blocks = [block for pair in zip(near, far) for block in pair]
    all_peaks = jnp.stack([near_peaks, far_peaks], axis=1)
    all_peaks = all_peaks.reshape((pj_count,) + peaks.shape)
    scale = jnp.exp(all_peaks - jnp.max(all_peaks, axis=0)[None])
    per_row = pj_count // pi_count
    weights_full, totals = join_call(blocks, jnp.transpose(scale, (1, 2, 0)), per_row)
    row_total = totals[:, 0, :]

    switch_share = jax.nn.sigmoid(
        jnp.einsum(
            "scn,ce->sen", rescaled_aligned, switch_weights, preferred_element_type=jnp.float32
        )
    )
    value_segment = jnp.einsum(
        "scn,ce->sen",
        jnp.concatenate(aligned_blocks, axis=2),
        payload_weights,
        preferred_element_type=jnp.float32,
    ).astype(jnp.bfloat16)
    payload_each_attender = value_segment.reshape(
        aligned_seq_tally, attender_tally, attender_span, value_segment.shape[2]
    )
    numerator = jnp.einsum(
        "hij,shcj->shci", weights_full, payload_each_attender, preferred_element_type=jnp.float32
    )
    gate_per_head = switch_share.reshape(
        aligned_seq_tally, attender_tally, attender_span, entry_tally
    )
    averaged_result = (gate_per_head * (numerator / row_total[None, :, None, :])).astype(
        jnp.bfloat16
    )
    averaged_result = averaged_result.reshape(aligned_seq_tally, inner_embed_size, entry_tally)
    return jnp.einsum(
        "ser,ec->scr", averaged_result, closing_weights, preferred_element_type=jnp.float32
    ).astype(jnp.bfloat16)


def solution(mesh):
    return jax.shard_map(
        functools.partial(body, mesh.shape["pi"], mesh.shape["pj"]),
        mesh=mesh,
        in_specs=(P("pi", "pj", None), P(), P("pj", None, "pi"), P(), P(), P(), P(), P()),
        out_specs=P("pj", None, "pi"),
        check_vma=False,
    )
```

```python
import functools

import jax
import jax.numpy as jnp
from jax import lax
from jax.experimental import pallas as pl
from jax.experimental.pallas import tpu as pltpu
from jax.sharding import PartitionSpec as P

EPS = 1e-05
NT = (((1,), (1,)), ((), ()))


def dot(a, b, dims=(((1,), (0,)), ((), ()))):
    return lax.dot_general(a, b, dims, preferred_element_type=jnp.float32)


def rescale_embedding(inputs, axis):
    row_mean = jnp.mean(inputs, axis=axis, keepdims=True)
    centred = inputs - row_mean
    variance = jnp.mean(centred * centred, axis=axis, keepdims=True)
    return centred * lax.rsqrt(variance + EPS)


def pair_kernel(x_ref, w_ref, e_ref, m_ref, hold):
    rows, cols, chans = x_ref.shape
    heads = w_ref.shape[0]
    step = pl.program_id(0)
    w = w_ref[...]
    w = w - jnp.mean(w, axis=1, keepdims=True)
    hi = w.astype(jnp.bfloat16).astype(jnp.float32)
    mid = (w - hi).astype(jnp.bfloat16).astype(jnp.float32)
    w3 = jnp.concatenate([hi, mid, w - hi - mid, jnp.zeros_like(w)], axis=0)
    w3 = w3.astype(jnp.bfloat16)
    x = x_ref[...].reshape(rows * cols, chans)
    mean = dot(x, jnp.ones((chans, chans), jnp.bfloat16)) * (1.0 / chans)
    centred = x.astype(jnp.float32) - mean
    square = centred * centred
    top = square.astype(jnp.bfloat16)
    rest = (square - top.astype(jnp.float32)).astype(jnp.bfloat16)
    ones = jnp.ones((2 * heads, 2 * chans), jnp.bfloat16)
    variance = dot(ones, jnp.concatenate([top, rest], axis=1), NT)[:heads] * (1.0 / chans)
    parts = dot(w3, x, NT)
    scores = parts[:heads] + (parts[heads : 2 * heads] + parts[2 * heads : 3 * heads])
    scores = scores * lax.rsqrt(variance + EPS)
    lane = lax.broadcasted_iota(jnp.int32, m_ref.shape, 1)
    peaks = m_ref[...]
    for k in range(rows):
        one = scores[:, k * cols : (k + 1) * cols]
        peak = jnp.max(one, axis=1, keepdims=True)
        hold[:, k, :] = jnp.exp(one - peak)
        peaks = jnp.where(lane == step * rows + k, peak, peaks)
    m_ref[...] = peaks
    e_ref[...] = hold[...].astype(jnp.bfloat16)


def pair_call(duo, weights_t, part, parts):
    rows, cols, chans = duo.shape
    rows = rows // parts
    heads = weights_t.shape[0]
    tile = 16
    return pl.pallas_call(
        pair_kernel,
        grid=(rows // tile,),
        in_specs=[
            pl.BlockSpec((tile, cols, chans), lambda i: (i + part * (rows // tile), 0, 0)),
            pl.BlockSpec((heads, chans), lambda i: (0, 0)),
        ],
        out_specs=[
            pl.BlockSpec((heads, tile, cols), lambda i: (0, i, 0)),
            pl.BlockSpec((heads, rows), lambda i: (0, 0)),
        ],
        out_shape=[
            jax.ShapeDtypeStruct((heads, rows, cols), jnp.bfloat16),
            jax.ShapeDtypeStruct((heads, rows), jnp.float32),
        ],
        scratch_shapes=[pltpu.VMEM((heads, tile, cols), jnp.float32)],
        compiler_params=pltpu.CompilerParams(
            dimension_semantics=("arbitrary",), vmem_limit_bytes=40 << 20
        ),
        cost_estimate=pl.CostEstimate(
            flops=4 * 10**9 // parts, bytes_accessed=duo.size * 2 // parts, transcendentals=0
        ),
        name="pair",
    )(duo, weights_t)


def join_kernel(per_row, *refs):
    *blocks, scale_ref, w_ref, total_ref = refs
    cols = blocks[0].shape[2]
    me_i, me_j = lax.axis_index("pi"), lax.axis_index("pj")
    for r, block in enumerate(blocks):
        owner = me_j ^ r
        place = (lax.div(owner, per_row) ^ me_i) * per_row + lax.rem(owner, per_row)
        scaled = block[0].astype(jnp.float32) * scale_ref[0][:, r : r + 1]
        w_ref[0, :, pl.ds(pl.multiple_of(place * cols, cols), cols)] = scaled.astype(jnp.bfloat16)
    total_ref[0] = dot(jnp.ones((8, w_ref.shape[2]), jnp.bfloat16), w_ref[0], NT)


def join_call(blocks, scale, per_row):
    heads, rows, cols = blocks[0].shape
    count = len(blocks)
    return pl.pallas_call(
        functools.partial(join_kernel, per_row),
        grid=(heads,),
        in_specs=[pl.BlockSpec((1, rows, cols), lambda h: (h, 0, 0))] * count
        + [pl.BlockSpec((1, rows, count), lambda h: (h, 0, 0))],
        out_specs=[
            pl.BlockSpec((1, rows, count * cols), lambda h: (h, 0, 0)),
            pl.BlockSpec((1, 8, rows), lambda h: (h, 0, 0)),
        ],
        out_shape=[
            jax.ShapeDtypeStruct((heads, rows, count * cols), jnp.bfloat16),
            jax.ShapeDtypeStruct((heads, 8, rows), jnp.float32),
        ],
        compiler_params=pltpu.CompilerParams(
            dimension_semantics=("arbitrary",), vmem_limit_bytes=24 << 20
        ),
        name="join",
    )(*blocks, scale)


def body(
    pi_count,
    pj_count,
    duo_embedding,
    duo_attention_weights,
    aligned_embedding,
    aligned_scaling_weights,
    aligned_shift_vector,
    payload_weights,
    switch_weights,
    closing_weights,
):
    attender_tally = duo_attention_weights.shape[1]
    entry_tally = duo_embedding.shape[0]
    aligned_seq_tally = aligned_embedding.shape[0]
    inner_embed_size = payload_weights.shape[1]
    attender_span = inner_embed_size // attender_tally

    def swap(array, axis, count, bit):
        return lax.ppermute(array, axis, [(q, q ^ bit) for q in range(count)])

    rescaled_aligned = (
        rescale_embedding(aligned_embedding.astype(jnp.float32), 1)
        * aligned_scaling_weights[None, :, None]
        + aligned_shift_vector[None, :, None]
    ).astype(jnp.bfloat16)
    aligned_blocks = [rescaled_aligned] + [
        swap(rescaled_aligned, "pi", pi_count, r) for r in range(1, pi_count)
    ]

    weights_t, rescaled_aligned = lax.optimization_barrier(
        (duo_attention_weights.T, rescaled_aligned)
    )
    parts = 2
    part_rows = entry_tally // parts
    per_row = pj_count // pi_count
    steps = range(2, pj_count, 2)
    sent = []
    for part in range(parts):
        exp_scores, peaks = pair_call(duo_embedding, weights_t, part, parts)
        weights_t, exp_scores, peaks = lax.optimization_barrier((weights_t, exp_scores, peaks))
        near_peaks = [peaks] + [swap(peaks, "pj", pj_count, r) for r in steps]
        near = [exp_scores] + [swap(exp_scores, "pj", pj_count, r) for r in steps]
        sent.append((near, near_peaks))

    def gather_rest(near, near_peaks):
        far = [swap(block, "pj", pj_count, 1) for block in near]
        near_peaks = jnp.stack(near_peaks)
        far_peaks = swap(near_peaks, "pj", pj_count, 1)
        blocks = [block for pair in zip(near, far) for block in pair]
        all_peaks = jnp.stack([near_peaks, far_peaks], axis=1)
        all_peaks = all_peaks.reshape((pj_count,) + near_peaks.shape[1:])
        scale = jnp.exp(all_peaks - jnp.max(all_peaks, axis=0)[None])
        return join_call(blocks, jnp.transpose(scale, (1, 2, 0)), per_row)

    switch_share = jax.nn.sigmoid(
        jnp.einsum(
            "scn,ce->sen", rescaled_aligned, switch_weights, preferred_element_type=jnp.float32
        )
    )
    value_segment = jnp.einsum(
        "scn,ce->sen",
        jnp.concatenate(aligned_blocks, axis=2),
        payload_weights,
        preferred_element_type=jnp.float32,
    ).astype(jnp.bfloat16)
    payload_each_attender = value_segment.reshape(
        aligned_seq_tally, attender_tally, attender_span, value_segment.shape[2]
    )
    gate_per_head = switch_share.reshape(
        aligned_seq_tally, attender_tally, attender_span, entry_tally
    )
    updates = []
    for part in range(parts):
        near, near_peaks = sent[part]
        if updates:
            updates[-1], near, near_peaks = lax.optimization_barrier(
                (updates[-1], near, near_peaks)
            )
        weights_full, totals = gather_rest(near, near_peaks)
        numerator = jnp.einsum(
            "hij,shcj->shci",
            weights_full,
            payload_each_attender,
            preferred_element_type=jnp.float32,
        )
        gate = gate_per_head[..., part * part_rows : (part + 1) * part_rows]
        averaged_result = (gate * (numerator / totals[None, :, :1, :])).astype(jnp.bfloat16)
        averaged_result = averaged_result.reshape(aligned_seq_tally, inner_embed_size, part_rows)
        updates.append(
            jnp.einsum(
                "ser,ec->scr", averaged_result, closing_weights, preferred_element_type=jnp.float32
            ).astype(jnp.bfloat16)
        )
    return jnp.concatenate(updates, axis=2)


def solution(mesh):
    return jax.shard_map(
        functools.partial(body, mesh.shape["pi"], mesh.shape["pj"]),
        mesh=mesh,
        in_specs=(P("pi", "pj", None), P(), P("pj", None, "pi"), P(), P(), P(), P(), P()),
        out_specs=P("pj", None, "pi"),
        check_vma=False,
    )
```
